32 devices in a mesh: cfg: 2 (over core), tp: 8 (over z, x), dp: 2 (over y).
Axes of the slice: x: 2, y: 2, z: 4, core: 2. Of those that a mesh axis runs over, the one named last changes fastest.
Arguments:
- tokens: bfloat16 [4096, 512], P('dp'), parts along dimension 0, may hold values from -6 to 6
- conditions: float32 [4, 256], P(('dp', 'cfg')), parts along dimension 0, may hold values from -6 to 6
- ada_block: bfloat16 [256, 3072], P(None, 'tp'), may hold values from -1 to 1
- ada_final: bfloat16 [256, 1024], P(None, 'tp'), may hold values from -1 to 1
- qkv_weight: bfloat16 [512, 3, 512], P(None, None, 'tp'), may hold values from -0.25 to 0.25
- out_weight: bfloat16 [512, 512], P('tp'), may hold values from -0.25 to 0.25
- up_weight: bfloat16 [512, 2048], P(None, 'tp'), may hold values from -0.25 to 0.25
- down_weight: bfloat16 [2048, 512], P('tp'), may hold values from -0.125 to 0.125
- final_weight: bfloat16 [512, 64], replicated, may hold values from -0.25 to 0.25
Outputs:
- guided: float32 [4096, 64], P('dp'), parts along dimension 0
The draws below stay inside these ranges and needn't reach their ends.
There are 2 independent parts, one for each index of `dp`. The reference program is written for one: setup_inputs(seed, part) draws one part's arguments, and reference() takes and returns one part's arrays. A program takes and returns all parts, laid end to end along the dimension named above; an argument that names none is the same for every part. Nothing has to cross between parts.
All inputs are finite; a program needn't handle non-finite values.
Results may differ from the reference program's by a relative error of at most 0.02.
Values may be sent and summed in bfloat16 or wider, within the bound.
A program may use at most 128 MiB of HBM per device.

```python
import jax
import jax.numpy as jnp
from jax import lax

HEAD_SIZE = 64
COND = 256
PATCH_OUT = 64
TOKENS = 2048
HEADS = 8
D = 512
FF = 2048


def level_of(stream_key, extent, pieces, smallest, top_value):
    def one(dim, shards_of):
        draws = jax.random.uniform(jax.random.fold_in(jax.random.fold_in(stream_key, 6), dim), (shards_of,), jnp.float32, smallest / len(pieces), top_value / len(pieces))
        return jnp.repeat(jnp.exp(draws), extent[dim] // shards_of).reshape((-1,) + (1,) * (len(extent) - dim - 1))

    gain = one(*pieces[0])
    for cut in pieces[1:]:
        gain = gain * one(*cut)
    return gain


def gaussian(own_key, shape, deviation, reach, split=(), dtype=jnp.bfloat16):
    drawn = deviation * jax.random.normal(own_key, shape, jnp.float32)
    if split:
        drawn = drawn * level_of(own_key, shape, split, -0.22, 0.18)
    return jnp.clip(drawn, -reach, reach).astype(dtype)


def setup_inputs(seed: int = 0, part: int = 0) -> dict:
    splits = jax.random.split(jax.random.key(seed), 10)
    own_keys = jax.random.split(jax.random.fold_in(splits[9], part), 10)
    tokens = gaussian(own_keys[0], (TOKENS, D), 1.0, 6.0)
    conditions = gaussian(own_keys[1], (2, COND), 1.0, 6.0, ((0, 2),), jnp.float32)
    ada_block = gaussian(splits[2], (COND, 6 * D), (COND // 8) ** -0.5, 1.0, ((1, 8),))
    ada_final = gaussian(splits[3], (COND, 2 * D), (COND // 8) ** -0.5, 1.0, ((1, 8),))
    qkv_weight = gaussian(splits[4], (D, 3, D), D ** -0.5, 0.25, ((2, 8),))
    out_weight = gaussian(splits[5], (D, D), D ** -0.5, 0.25, ((0, 8),))
    up_weight = gaussian(splits[6], (D, FF), D ** -0.5, 0.25, ((1, 8),))
    down_weight = gaussian(splits[7], (FF, D), FF ** -0.5, 0.125, ((0, 8),))
    final_weight = gaussian(splits[8], (D, PATCH_OUT), D ** -0.5, 0.25)
    return dict(tokens=tokens, conditions=conditions, ada_block=ada_block, ada_final=ada_final, qkv_weight=qkv_weight, out_weight=out_weight, up_weight=up_weight, down_weight=down_weight, final_weight=final_weight)


guidance = 4.0
epsilon = 1e-06

def layer_norm(values):
    average = lax.optimization_barrier(jnp.mean(values, -1, keepdims=True))
    centred = values - average
    spread = lax.optimization_barrier(jnp.mean(centred * centred, -1, keepdims=True))
    return centred * lax.rsqrt(spread + epsilon)

def modulate(stream, scales, shifts):
    return (layer_norm(stream) * (1.0 + scales) + shifts).astype(jnp.bfloat16)

def branch(tokens, cond_row, ada_block, ada_final, qkv_weight, out_weight, up_weight, down_weight, final_weight):
    model_width = tokens.shape[1]
    signal = jax.nn.silu(cond_row).astype(jnp.bfloat16)[None, :]
    shifts = jnp.dot(signal, ada_block, preferred_element_type=jnp.float32)[0].reshape(6, model_width)
    final_mod = jnp.dot(signal, ada_final, preferred_element_type=jnp.float32)[0].reshape(2, model_width)
    stream = tokens.astype(jnp.float32)
    normed = modulate(stream, shifts[1], shifts[0])
    projected = jnp.einsum('td,dke->tke', normed.astype(jnp.float32), qkv_weight.astype(jnp.float32)).astype(jnp.bfloat16)
    per_head = projected.reshape(TOKENS, 3, HEADS, HEAD_SIZE).astype(jnp.float32)
    scores = jnp.einsum('thd,shd->hts', per_head[:, 0], per_head[:, 1]) * HEAD_SIZE ** (-0.5)
    softmaxed = jax.nn.softmax(scores, axis=-1)
    head_out = jnp.einsum('hts,shd->thd', softmaxed, per_head[:, 2]).reshape(TOKENS, model_width).astype(jnp.bfloat16)
    attended = jnp.dot(head_out, out_weight, preferred_element_type=jnp.float32)
    stream = stream + shifts[2] * attended
    normed = modulate(stream, shifts[4], shifts[3])
    hidden = jax.nn.gelu(jnp.dot(normed, up_weight, preferred_element_type=jnp.float32), approximate=True).astype(jnp.bfloat16)
    mlp_out = jnp.dot(hidden, down_weight, preferred_element_type=jnp.float32)
    stream = stream + shifts[5] * mlp_out
    final_in = modulate(stream, final_mod[1], final_mod[0])
    return jnp.dot(final_in, final_weight, preferred_element_type=jnp.float32)

def reference(tokens, conditions, ada_block, ada_final, qkv_weight, out_weight, up_weight, down_weight, final_weight):
    guided_on = branch(tokens, conditions[0], ada_block, ada_final, qkv_weight, out_weight, up_weight, down_weight, final_weight)
    guided_off = branch(tokens, conditions[1], ada_block, ada_final, qkv_weight, out_weight, up_weight, down_weight, final_weight)
    return guidance * guided_on + (1.0 - guidance) * guided_off
```

```python
import functools
import math

import jax
import jax.numpy as jnp
from jax import lax
from jax.experimental import pallas as pl
from jax.experimental.pallas import tpu as pltpu
from jax.sharding import PartitionSpec as P

HEAD_SIZE = 64
MESH = pl.DeviceIdType.MESH
F32, BF16 = jnp.float32, jnp.bfloat16

guidance = 4.0
epsilon = 1e-06


def layer_norm(values):
    average = jnp.mean(values, -1, keepdims=True)
    centred = values - average
    spread = jnp.mean(centred * centred, -1, keepdims=True)
    return centred * lax.rsqrt(spread + epsilon)


def modulate(stream, scales, shifts):
    return (layer_norm(stream) * (1.0 + scales) + shifts).astype(BF16)


def dot(a, b):
    return jnp.dot(a, b, preferred_element_type=F32)


def dot_nt(a, b):
    return lax.dot_general(a, b, (((1,), (1,)), ((), ())), preferred_element_type=F32)


def remote(src, dst, send, recv, where):
    return pltpu.make_async_remote_copy(
        src_ref=src, dst_ref=dst, send_sem=send, recv_sem=recv, device_id=where, device_id_type=MESH
    )


def rows_of(ref, start, count):
    return ref.at[pl.ds(pl.multiple_of(start, count), count)]


def block_kernel(
    n,
    tokens, cond, ada_block, ada_final, qkv, out_w, up_w, down_w, final_w,
    result,
    mod_mine, mod_all, xhat, q_s, k_s, v_s, ho_mine, ho_all, f_out, f_up, f_down,
    half_out, half_in, fin_buf,
    mod_send, mod_recv, ho_send, ho_recv, g_send, g_recv, h_sem, p_send, p_recv, d_send, d_recv,
):
    me = lax.axis_index("tp")
    c = lax.axis_index("cfg")
    other = {"cfg": 1 - c}
    count, width = tokens.shape
    shard = count // n
    nz = n // 2
    x, z = lax.rem(me, 2), me // 2

    def at(col, dz):
        return lax.rem(z + dz + nz, nz) * 2 + lax.rem(x + col, 2)

    barrier = pltpu.get_barrier_semaphore()
    for d in range(1, n):
        pl.semaphore_signal(
            barrier, inc=1, device_id={"tp": lax.rem(me + d, n)}, device_id_type=MESH
        )
    pl.semaphore_signal(barrier, inc=1, device_id=other, device_id_type=MESH)

    raw = cond[...]
    signal = jnp.broadcast_to(raw / (1.0 + jnp.exp(-raw)), (8, raw.shape[1])).astype(BF16)
    nb, nf = ada_block.shape[1], ada_final.shape[1]
    mod_mine[0, :, :nb] = dot(signal, ada_block[...])[0:1]
    mod_mine[0, :, nb:] = dot(signal, ada_final[...])[0:1]
    pl.semaphore_wait(barrier, n)

    def mod_copy(d):
        return remote(
            mod_mine.at[0], mod_all.at[me], mod_send.at[d - 1], mod_recv.at[d - 1],
            {"tp": lax.rem(me + d, n)},
        )

    for d in range(1, n):
        mod_copy(d).start()

    own = (out_w, up_w, down_w)
    full = (f_out, f_up, f_down)
    places = [
        (at(1, 0), 0), (at(0, -1), 0), (at(0, 1), 0), (at(1, -1), 0), (at(1, 1), 0),
        (at(0, 2), 1), (at(0, 2), 2), (at(1, 2), 1), (at(1, 2), 2),
    ]

    def region(ref, part, core):
        rows = ref.shape[0]
        if part == 0:
            return rows_of(ref, core * (rows // 2), rows // 2)
        return rows_of(ref, core * (rows // 2) + (part - 1) * (rows // 4), rows // 4)

    plus, minus, across = {"tp": at(0, 1)}, {"tp": at(0, -1)}, {"tp": at(1, 0)}
    sends = [
        (me, 0, across), (me, 0, plus), (me, 0, minus),
        (at(1, 0), 0, plus), (at(1, 0), 0, minus),
        (at(0, -1), 1, plus), (at(0, 1), 2, minus),
        (at(1, -1), 1, plus), (at(1, 1), 2, minus),
    ]
    links = len(sends)

    def link(k, j):
        owner, part, where = sends[j]
        src = own[k] if j < 3 else full[k].at[owner]
        return remote(
            region(src, part, c), region(full[k].at[owner], part, c),
            g_send.at[k, j], g_recv.at[k, j], where,
        )

    def landed(k, j):
        owner, part = places[j]
        dst = region(full[k].at[owner], part, c)
        return remote(dst, dst, g_send.at[k, j], g_recv.at[k, j], across)

    def share(k, j):
        owner, part = places[j]
        dst = region(full[k].at[owner], part, c)
        return remote(dst, dst, g_send.at[k, links + j], g_recv.at[k, links + j], other)

    def shared(k, j):
        owner, part = places[j]
        dst = region(full[k].at[owner], part, 1 - c)
        return remote(dst, dst, g_send.at[k, links + j], g_recv.at[k, links + j], other)

    def open_gather(k):
        for j in (0, 1, 2):
            link(k, j).start()

    def forward(k, arrivals, starts):
        for j in arrivals:
            landed(k, j).wait_recv()
        for j in starts:
            link(k, j).start()
        for j in arrivals:
            share(k, j).start()

    open_gather(0)
    open_gather(1)
    for k in range(3):
        full[k][me] = own[k][...]

    def norm_step(i, _):
        r = pl.ds(pl.multiple_of(i * shard, shard), shard)
        xhat[r, :] = layer_norm(tokens[r, :].astype(F32))
        return 0

    lax.fori_loop(0, count // shard, norm_step, 0)

    mod_all[me] = mod_mine[0]
    for d in range(1, n):
        origin = mod_all.at[lax.rem(me - d + n, n)]
        remote(origin, origin, mod_send.at[d - 1], mod_recv.at[d - 1], across).wait_recv()

    def mod_row(base, per, row):
        lane = math.gcd(per, width)
        pieces = []
        for g in range(row * width // lane, (row + 1) * width // lane):
            t, off = (g * lane) // per, (g * lane) % per
            pieces.append(mod_all[t, :, base + off : base + off + lane])
        return jnp.concatenate(pieces, axis=1)

    shift1, scale1, gate1, shift2, scale2, gate2 = [mod_row(0, nb, r) for r in range(6)]
    shift_f, scale_f = [mod_row(nb, nf, r) for r in range(2)]

    h = HEAD_SIZE
    ones = (lax.broadcasted_iota(jnp.int32, (shard, h), 1) == 0).astype(F32).astype(BF16)

    def qkv_step(i, _):
        r = pl.ds(pl.multiple_of(i * shard, shard), shard)
        normed = (xhat[r, :] * (1.0 + scale1) + shift1).astype(BF16)
        q_s[r, :] = (dot(normed, qkv[0]) * (h ** -0.5 * math.log2(math.e))).astype(BF16)
        k_s[r, :] = dot(normed, qkv[1]).astype(BF16)
        v_s[r, :h] = dot(normed, qkv[2]).astype(BF16)
        v_s[r, h:] = ones
        return 0

    lax.fori_loop(0, count // shard, qkv_step, 0)

    def ho_copy(i):
        return remote(
            ho_mine.at[i], ho_all.at[me], ho_send.at[i], ho_recv.at[i],
            {"tp": lax.rem(me + 1 + i, n)},
        )

    sub = shard // 2

    def attend_step(i, _):
        @pl.when(i == 0)
        def _():
            for k in (0, 1):
                forward(k, (0, 1, 2), (3, 4, 5, 6))
            open_gather(2)

        @pl.when(i == 3)
        def _():
            for k in (0, 1):
                forward(k, (3, 4), (7, 8))

        @pl.when(i == 4)
        def _():
            forward(2, (0, 1, 2), (3, 4, 5, 6))
            for k in (0, 1):
                forward(k, (5, 6), ())

        @pl.when(i == 6)
        def _():
            forward(2, (3, 4), (7, 8))
            for k in (0, 1):
                forward(k, (7, 8), ())

        peer = lax.rem(me + 1 + i, n)
        for part in range(shard // sub):
            r = pl.ds(pl.multiple_of(peer * shard + part * sub, sub), sub)
            scores = dot_nt(q_s[r, :], k_s[...])
            top = jnp.max(scores, axis=-1, keepdims=True)
            weights = jnp.exp2(scores - top).astype(BF16)
            mixed = dot(weights, v_s[...])
            ho_mine[i, part * sub : (part + 1) * sub, :] = (
                mixed[:, :h] / mixed[:, h : h + 1]
            ).astype(BF16)

        @pl.when(i < n - 1)
        def _():
            ho_copy(i).start()

        return 0

    lax.fori_loop(0, n, attend_step, 0)
    forward(2, (5, 6), ())

    ho_all[me] = ho_mine[n - 1]
    for j in range(links):
        shared(0, j).wait_recv()
    for i in range(n - 1):
        origin = ho_all.at[lax.rem(me - 1 - i + n, n)]
        remote(origin, origin, ho_send.at[i], ho_recv.at[i], across).wait_recv()
    attended = dot(ho_all[0], f_out[0])
    for t in range(1, n):
        attended += dot(ho_all[t], f_out[t])
    r = pl.ds(pl.multiple_of(me * shard, shard), shard)
    stream = tokens[r, :].astype(F32) + gate1 * attended
    normed = modulate(stream, scale2, shift2)
    forward(2, (7, 8), ())
    for j in range(links):
        shared(1, j).wait_recv()
    hidden = [
        jax.nn.gelu(dot(normed, f_up[t]), approximate=True).astype(BF16) for t in range(n)
    ]
    for j in range(links):
        shared(2, j).wait_recv()
    mlp = dot(hidden[0], f_down[0])
    for t in range(1, n):
        mlp += dot(hidden[t], f_down[t])
    stream = stream + gate2 * mlp
    final_in = modulate(stream, scale_f, shift_f)

    weighting = jnp.where(c == 0, guidance, 1.0 - guidance).astype(F32)
    out_width = final_w.shape[1]
    predicted = weighting * dot(final_in, final_w[...])
    quarter = shard // 4
    for half in range(2):
        lo = half * 2 * quarter
        half_out[half, :, :] = jnp.concatenate(
            [predicted[lo : lo + quarter], predicted[lo + quarter : lo + 2 * quarter]], axis=1
        )
    trade = remote(half_out.at[1 - c], half_in, h_sem.at[0], h_sem.at[1], other)
    trade.start()
    trade.wait()
    fin_buf[me, c] = (half_out[c] + half_in[...]).astype(BF16)

    def push(d):
        return remote(
            fin_buf.at[me, c], fin_buf.at[me, c], p_send.at[d], p_recv.at[d],
            {"tp": lax.rem(me + d, n)},
        )

    def hand(d, core):
        place = fin_buf.at[lax.rem(me - d + n, n), core]
        return remote(place, place, d_send.at[d], d_recv.at[d], other)

    for d in (4, 3, 5, 2, 6, 1, 7):
        if d < n:
            push(d).start()
    hand(0, c).start()
    for d in range(1, n):
        place = fin_buf.at[lax.rem(me - d + n, n), c]
        remote(place, place, p_send.at[d], p_recv.at[d], across).wait_recv()
        hand(d, c).start()
    for d in range(n):
        hand(d, 1 - c).wait_recv()
    for t in range(n):
        for half in range(2):
            both = fin_buf[t, half].astype(F32)
            lo = t * shard + half * 2 * quarter
            result[lo : lo + quarter, :] = both[:, :out_width]
            result[lo + quarter : lo + 2 * quarter, :] = both[:, out_width:]

    for d in range(1, n):
        mod_copy(d).wait_send()
        push(d).wait_send()
        ho_copy(d - 1).wait_send()
    for d in range(n):
        hand(d, c).wait_send()
    for k in range(3):
        for j in range(links):
            link(k, j).wait_send()
            share(k, j).wait_send()


def fused(n, tokens, cond, ada_block, ada_final, qkv_weight, out_weight, up_weight, down_weight, final_weight):
    count, width = tokens.shape
    shard = count // n
    qkv = jnp.transpose(qkv_weight, (1, 0, 2))
    mod = ada_block.shape[1] + ada_final.shape[1]
    h, out_width = HEAD_SIZE, final_weight.shape[1]
    dma = pltpu.SemaphoreType.DMA
    vm = pl.BlockSpec(memory_space=pltpu.VMEM)
    return pl.pallas_call(
        functools.partial(block_kernel, n),
        out_shape=jax.ShapeDtypeStruct((count, out_width), F32),
        in_specs=[vm] * 9,
        out_specs=vm,
        scratch_shapes=[
            pltpu.VMEM((1, 1, mod), F32),
            pltpu.VMEM((n, 1, mod), F32),
            pltpu.VMEM((count, width), F32),
            pltpu.VMEM((count, h), BF16),
            pltpu.VMEM((count, h), BF16),
            pltpu.VMEM((count, 2 * h), BF16),
            pltpu.VMEM((n, shard, h), BF16),
            pltpu.VMEM((n, shard, h), BF16),
            pltpu.VMEM((n,) + out_weight.shape, BF16),
            pltpu.VMEM((n,) + up_weight.shape, BF16),
            pltpu.VMEM((n,) + down_weight.shape, BF16),
            pltpu.VMEM((2, shard // 4, 2 * out_width), F32),
            pltpu.VMEM((shard // 4, 2 * out_width), F32),
            pltpu.VMEM((n, 2, shard // 4, 2 * out_width), BF16),
            dma((n - 1,)), dma((n - 1,)),
            dma((n - 1,)), dma((n - 1,)),
            dma((3, 18)), dma((3, 18)),
            dma((2,)),
            dma((n,)), dma((n,)),
            dma((n,)), dma((n,)),
        ],
        compiler_params=pltpu.CompilerParams(
            collective_id=0, has_side_effects=True, vmem_limit_bytes=60 * 1024 * 1024
        ),
    )(tokens, cond, ada_block, ada_final, qkv, out_weight, up_weight, down_weight, final_weight)


def attend(projected):
    token_count = projected.shape[0]
    local_width = projected.shape[2]
    local_heads = local_width // HEAD_SIZE
    per_head = projected.reshape(token_count, 3, local_heads, HEAD_SIZE)
    scores = jnp.einsum(
        "thd,shd->hts", per_head[:, 0], per_head[:, 1], preferred_element_type=jnp.float32
    ) * HEAD_SIZE ** (-0.5)
    softmaxed = jax.nn.softmax(scores, axis=-1)
    values_f = per_head[:, 2].astype(jnp.float32)
    head_out = jnp.einsum("hts,shd->thd", softmaxed, values_f)
    return head_out.reshape(token_count, local_width).astype(jnp.bfloat16)


def split(
    tokens,
    conditions,
    ada_block,
    ada_final,
    qkv_weight,
    out_weight,
    up_weight,
    down_weight,
    final_weight,
):
    model_width = tokens.shape[1]
    signal = jax.nn.silu(conditions).astype(jnp.bfloat16)
    block_local = jnp.dot(signal, ada_block, preferred_element_type=jnp.float32)[0]
    final_local = jnp.dot(signal, ada_final, preferred_element_type=jnp.float32)[0]
    shifts, final_mod = (
        lax.all_gather(block_local, "tp", axis=0, tiled=True),
        lax.all_gather(final_local, "tp", axis=0, tiled=True),
    )
    shifts = shifts.reshape(6, model_width)
    stream = tokens.astype(jnp.float32)
    normed = modulate(stream, shifts[1], shifts[0])
    projected = jnp.einsum(
        "td,dke->tke", normed, qkv_weight, preferred_element_type=jnp.float32
    ).astype(jnp.bfloat16)
    head_out = attend(projected)
    attended = lax.psum(
        jnp.dot(head_out, out_weight, preferred_element_type=jnp.float32).astype(jnp.bfloat16), "tp"
    ).astype(jnp.float32)
    stream = stream + shifts[2] * attended
    normed = modulate(stream, shifts[4], shifts[3])
    upward = jnp.dot(normed, up_weight, preferred_element_type=jnp.float32)
    hidden = jax.nn.gelu(upward, approximate=True).astype(jnp.bfloat16)
    mlp_out = lax.psum(
        jnp.dot(hidden, down_weight, preferred_element_type=jnp.float32).astype(jnp.bfloat16), "tp"
    ).astype(jnp.float32)
    stream = stream + shifts[5] * mlp_out
    final_mod = final_mod.reshape(2, model_width)
    final_in = modulate(stream, final_mod[1], final_mod[0])
    predicted = jnp.dot(final_in, final_weight, preferred_element_type=jnp.float32)
    is_cond = lax.axis_index("cfg") == 0
    weighting = jnp.where(is_cond, guidance, 1.0 - guidance).astype(jnp.float32)
    return lax.psum((weighting * predicted).astype(jnp.bfloat16), "cfg").astype(jnp.float32)


def solution(mesh):
    n = mesh.shape["tp"]

    def local(tokens, cond, ada_block, ada_final, qkv_weight, out_weight, up_weight, down_weight, final_weight):
        args = (tokens, cond, ada_block, ada_final, qkv_weight, out_weight, up_weight, down_weight, final_weight)
        gathered = 2 * n * (out_weight.size + up_weight.size + down_weight.size)
        needed = gathered + 8 * tokens.size + 16 * tokens.shape[0] * HEAD_SIZE
        one_head = qkv_weight.shape[2] == HEAD_SIZE
        fits = needed < 24 * 1024 * 1024 and tokens.shape[0] % (64 * n) == 0
        if n == 8 and mesh.shape["cfg"] == 2 and one_head and fits:
            return fused(n, *args)
        return split(*args)

    placed = (
        P("dp", None),
        P(("dp", "cfg"), None),
        P(None, "tp"),
        P(None, "tp"),
        P(None, None, "tp"),
        P("tp", None),
        P(None, "tp"),
        P("tp", None),
        P(),
    )
    return jax.shard_map(
        local, mesh=mesh, in_specs=placed, out_specs=P("dp", None), check_vma=False
    )
```

```python
import functools
import math

import jax
import jax.numpy as jnp
from jax import lax
from jax.experimental import pallas as pl
from jax.experimental.pallas import tpu as pltpu
from jax.sharding import PartitionSpec as P

HEAD_SIZE = 64
MESH = pl.DeviceIdType.MESH
F32, BF16 = jnp.float32, jnp.bfloat16

PLAN = {
    0: ((0, 1), (1, 1)),
    1: ((2, 1),),
    2: ((0, 2), (1, 2)),
    4: ((2, 2), (0, 3)),
    5: ((1, 3),),
    6: ((2, 3), (0, 4)),
}
LATE = ((1, 4), (2, 4))

guidance = 4.0
epsilon = 1e-06


def layer_norm(values):
    average = jnp.mean(values, -1, keepdims=True)
    centred = values - average
    spread = jnp.mean(centred * centred, -1, keepdims=True)
    return centred * lax.rsqrt(spread + epsilon)


def modulate(stream, scales, shifts):
    return (layer_norm(stream) * (1.0 + scales) + shifts).astype(BF16)


def dot(a, b):
    return jnp.dot(a, b, preferred_element_type=F32)


def dot_nt(a, b):
    return lax.dot_general(a, b, (((1,), (1,)), ((), ())), preferred_element_type=F32)


def remote(src, dst, send, recv, where):
    return pltpu.make_async_remote_copy(
        src_ref=src, dst_ref=dst, send_sem=send, recv_sem=recv, device_id=where, device_id_type=MESH
    )


def rows_of(ref, start, count):
    return ref.at[pl.ds(pl.multiple_of(start, count), count)]


def block_kernel(
    n,
    tokens, cond, ada_block, ada_final, qkv, out_w, up_w, down_w, final_w,
    result,
    mod_mine, mod_all, xhat, q_s, k_s, v_s, ho_mine, ho_all, f_out, f_up, f_down,
    half_out, half_in, fin_buf,
    mod_send, mod_recv, ho_send, ho_recv, z_send, z_recv, x_send, x_recv, y_send, y_recv, s_send, s_recv, h_sem, p_send, p_recv, d_send, d_recv,
):
    me = lax.axis_index("tp")
    c = lax.axis_index("cfg")
    other = {"cfg": 1 - c}
    count, width = tokens.shape
    shard = count // n
    nz = n // 2
    x, z = lax.rem(me, 2), me // 2

    y = lax.axis_index("dp")
    beside = {"dp": 1 - y}
    across = {"tp": z * 2 + 1 - x}

    barrier = pltpu.get_barrier_semaphore()
    for d in range(1, n):
        pl.semaphore_signal(
            barrier, inc=1, device_id={"tp": lax.rem(me + d, n)}, device_id_type=MESH
        )
    pl.semaphore_signal(barrier, inc=1, device_id=other, device_id_type=MESH)
    pl.semaphore_signal(barrier, inc=1, device_id=beside, device_id_type=MESH)

    raw = cond[...]
    signal = jnp.broadcast_to(raw / (1.0 + jnp.exp(-raw)), (8, raw.shape[1])).astype(BF16)
    nb, nf = ada_block.shape[1], ada_final.shape[1]
    mod_mine[0, :, :nb] = dot(signal, ada_block[...])[0:1]
    mod_mine[0, :, nb:] = dot(signal, ada_final[...])[0:1]
    pl.semaphore_wait(barrier, n + 1)

    def mod_copy(d):
        return remote(
            mod_mine.at[0], mod_all.at[me], mod_send.at[d - 1], mod_recv.at[d - 1],
            {"tp": lax.rem(me + d, n)},
        )

    for d in range(1, n):
        mod_copy(d).start()

    own = (out_w, up_w, down_w)
    full = (f_out, f_up, f_down)
    h = HEAD_SIZE

    def region(ref, k, core, plane=None):
        base, rows = 0, own[k].shape[0]
        if k == 0 and ref is not out_w:
            base = h
        size = rows // 2
        start = base + core * size
        if plane is not None:
            size = size // 2
            start = start + plane * size
        return rows_of(ref, start, size)

    def fetched(k, owner):
        return region(full[k].at[owner], k, c, y if k == 2 else None)

    def z_copy(k, zo, way, mine=False):
        owner = zo * 2 + x
        src = region(own[k], k, c, y if k == 2 else None) if mine else fetched(k, owner)
        return remote(
            src, fetched(k, owner), z_send.at[k, zo, way], z_recv.at[k, zo],
            {"tp": (z + 1 - 2 * way) * 2 + x},
        )

    def x_copy(k, zo, mine=False):
        owner = zo * 2 + x
        src = region(own[k], k, c, y if k == 2 else None) if mine else fetched(k, owner)
        return remote(src, fetched(k, owner), x_send.at[k, zo], x_recv.at[k, zo], across)

    def y_copy(owner, plane):
        dst = region(f_down.at[owner], 2, c, plane)
        return remote(dst, dst, y_send.at[owner], y_recv.at[owner], beside)

    def core_copy(k, owner, core):
        dst = region(full[k].at[owner], k, core)
        return remote(dst, dst, s_send.at[k, owner], s_recv.at[k, owner], other)

    def hand_on(k, owner):
        if k == 2:
            y_copy(owner, y).start()
        else:
            core_copy(k, owner, c).start()

    def stage(k, dist):
        if dist == 0:
            for way in (0, 1):
                @pl.when(z < nz - 1 if way == 0 else z > 0)
                def _():
                    z_copy(k, z, way, True).start()
            x_copy(k, z, True).start()
            return
        for way in (0, 1):
            zo = z - dist if way == 0 else z + dist
            inside = zo >= 0 if way == 0 else zo < nz

            if dist < nz:
                @pl.when(inside)
                def _():
                    z_copy(k, zo, way).wait_recv()
                    @pl.when(z < nz - 1 if way == 0 else z > 0)
                    def _():
                        z_copy(k, zo, way).start()
                    x_copy(k, zo).start()
                    hand_on(k, zo * 2 + x)

            zx = z - dist + 1 if way == 0 else z + dist - 1
            if dist > 1 or way == 0:
                @pl.when(zx >= 0 if way == 0 else zx < nz)
                def _():
                    place = fetched(k, zx * 2 + 1 - x)
                    remote(place, place, x_send.at[k, zx], x_recv.at[k, zx], across).wait_recv()
                    hand_on(k, zx * 2 + 1 - x)

    def share_down():
        for d in range(1, n):
            owner = lax.rem(me + d, n)
            y_copy(owner, 1 - y).wait_recv()
            core_copy(2, owner, c).start()

    def arrived(k):
        for d in range(1, n):
            core_copy(k, lax.rem(me + d, n), 1 - c).wait_recv()

    for k in range(3):
        stage(k, 0)
    empty = jnp.zeros((h, width), BF16)
    for t in range(n):
        f_out[t, :h] = empty
        f_out[t, 2 * h :] = empty
    f_out[me, h : 2 * h] = out_w[...]
    f_up[me] = up_w[...]
    f_down[me] = down_w[...]

    def norm_step(i, _):
        r = pl.ds(pl.multiple_of(i * shard, shard), shard)
        xhat[r, :] = layer_norm(tokens[r, :].astype(F32))
        return 0

    lax.fori_loop(0, count // shard, norm_step, 0)

    mod_all[me] = mod_mine[0]
    for d in range(1, n):
        origin = mod_all.at[lax.rem(me - d + n, n)]
        remote(origin, origin, mod_send.at[d - 1], mod_recv.at[d - 1], across).wait_recv()

    def mod_row(base, per, row):
        lane = math.gcd(per, width)
        pieces = []
        for g in range(row * width // lane, (row + 1) * width // lane):
            t, off = (g * lane) // per, (g * lane) % per
            pieces.append(mod_all[t, :, base + off : base + off + lane])
        return jnp.concatenate(pieces, axis=1)

    shift1, scale1, gate1, shift2, scale2, gate2 = [mod_row(0, nb, r) for r in range(6)]
    shift_f, scale_f = [mod_row(nb, nf, r) for r in range(2)]

    lanes = lax.broadcasted_iota(jnp.int32, (shard, 2 * h), 1)
    upper = (lanes >= h).astype(F32)
    v_w, none = qkv[2], jnp.zeros((h, width), BF16)
    v_low = jnp.concatenate([v_w, none], axis=0)
    v_high = jnp.concatenate([none, v_w], axis=0)

    def qkv_step(i, _):
        r = pl.ds(pl.multiple_of(i * shard, shard), shard)
        normed = (xhat[r, :] * (1.0 + scale1) + shift1).astype(BF16)
        q_s[r, :] = (dot_nt(normed, qkv[0]) * (h ** -0.5 * math.log2(math.e))).astype(BF16)
        k_s[r, :] = dot_nt(normed, qkv[1]).astype(BF16)
        v_s[0, r, :] = (dot_nt(normed, v_low) + upper).astype(BF16)
        v_s[1, r, :] = (dot_nt(normed, v_high) + (1.0 - upper)).astype(BF16)
        return 0

    lax.fori_loop(0, count // shard, qkv_step, 0)

    def ho_copy(i):
        return remote(
            ho_mine.at[i], ho_all.at[me], ho_send.at[i], ho_recv.at[i],
            {"tp": lax.rem(me + 1 + i, n)},
        )

    sub = shard // 2

    def attend_step(i, _):
        for when, steps in PLAN.items():
            @pl.when(i == when)
            def _():
                for k, dist in steps:
                    stage(k, dist)

        peer = lax.rem(me + 1 + i, n)
        parts = []
        for part in range(2):
            r = pl.ds(pl.multiple_of(peer * shard + part * sub, sub), sub)
            scores = dot_nt(q_s[r, :], k_s[...])
            top = jnp.max(scores, axis=-1, keepdims=True)
            weights = jnp.exp2(scores - top).astype(BF16)
            mixed = dot(weights, v_s[part])
            total = mixed[:, h : h + 1] if part == 0 else mixed[:, 0:1]
            parts.append(mixed / total)
        ho_mine[i] = jnp.where(lanes[:sub] < h, parts[0], parts[1]).astype(BF16)

        @pl.when(i < n - 1)
        def _():
            ho_copy(i).start()

        return 0

    lax.fori_loop(0, n, attend_step, 0)
    for k, dist in LATE:
        stage(k, dist)

    ho_all[me] = ho_mine[n - 1]
    arrived(0)
    for i in range(n - 1):
        origin = ho_all.at[lax.rem(me - 1 - i + n, n)]
        remote(origin, origin, ho_send.at[i], ho_recv.at[i], across).wait_recv()
    def project(lo):
        sums = dot(ho_all[0], f_out[0, lo : lo + 2 * h])
        for t in range(1, n):
            sums += dot(ho_all[t], f_out[t, lo : lo + 2 * h])
        return sums

    attended = jnp.concatenate([project(h), project(0)], axis=0)
    r = pl.ds(pl.multiple_of(me * shard, shard), shard)
    stream = tokens[r, :].astype(F32) + gate1 * attended
    normed = modulate(stream, scale2, shift2)
    share_down()
    arrived(1)
    hidden = [
        jax.nn.gelu(dot(normed, f_up[t]), approximate=True).astype(BF16) for t in range(n)
    ]
    arrived(2)
    mlp = dot(hidden[0], f_down[0])
    for t in range(1, n):
        mlp += dot(hidden[t], f_down[t])
    stream = stream + gate2 * mlp
    final_in = modulate(stream, scale_f, shift_f)

    weighting = jnp.where(c == 0, guidance, 1.0 - guidance).astype(F32)
    predicted = weighting * dot_nt(final_w[...], final_in)
    part = shard // 2
    for half in range(2):
        half_out[half] = predicted[:, half * part : (half + 1) * part]
    trade = remote(half_out.at[1 - c], half_in, h_sem.at[0], h_sem.at[1], other)
    trade.start()
    trade.wait()
    fin_buf[me, c] = (half_out[c] + half_in[...]).astype(BF16)

    def push(d):
        return remote(
            fin_buf.at[me, c], fin_buf.at[me, c], p_send.at[d], p_recv.at[d],
            {"tp": lax.rem(me + d, n)},
        )

    def hand(d, core):
        place = fin_buf.at[lax.rem(me - d + n, n), core]
        return remote(place, place, d_send.at[d], d_recv.at[d], other)

    for d in (4, 3, 5, 2, 6, 1, 7):
        if d < n:
            push(d).start()
    hand(0, c).start()
    for d in range(1, n):
        place = fin_buf.at[lax.rem(me - d + n, n), c]
        remote(place, place, p_send.at[d], p_recv.at[d], across).wait_recv()
        hand(d, c).start()
    for d in range(n):
        hand(d, 1 - c).wait_recv()
    for t in range(n):
        for half in range(2):
            lo = t * shard + half * part
            result[:, lo : lo + part] = fin_buf[t, half]

    for d in range(1, n):
        mod_copy(d).wait_send()
        push(d).wait_send()
        ho_copy(d - 1).wait_send()
    for d in range(n):
        hand(d, c).wait_send()
    for k in range(3):
        for zo in range(nz):
            x_copy(k, zo).wait_send()
        for way in (0, 1):
            @pl.when(z < nz - 1 if way == 0 else z > 0)
            def _():
                for dist in range(nz):
                    zo = z - dist if way == 0 else z + dist
                    @pl.when(zo >= 0 if way == 0 else zo < nz)
                    def _():
                        z_copy(k, zo, way).wait_send()
        for d in range(1, n):
            core_copy(k, lax.rem(me + d, n), c).wait_send()
    for d in range(1, n):
        y_copy(lax.rem(me + d, n), y).wait_send()


def fused(n, tokens, cond, ada_block, ada_final, qkv_weight, out_weight, up_weight, down_weight, final_weight):
    count, width = tokens.shape
    shard = count // n
    qkv = jnp.transpose(qkv_weight, (1, 2, 0))
    mod = ada_block.shape[1] + ada_final.shape[1]
    h, out_width = HEAD_SIZE, final_weight.shape[1]
    dma = pltpu.SemaphoreType.DMA
    vm = pl.BlockSpec(memory_space=pltpu.VMEM)
    guided = pl.pallas_call(
        functools.partial(block_kernel, n),
        out_shape=jax.ShapeDtypeStruct((out_width, count), BF16),
        in_specs=[vm] * 9,
        out_specs=vm,
        scratch_shapes=[
            pltpu.VMEM((1, 1, mod), F32),
            pltpu.VMEM((n, 1, mod), F32),
            pltpu.VMEM((count, width), F32),
            pltpu.VMEM((count, h), BF16),
            pltpu.VMEM((count, h), BF16),
            pltpu.VMEM((2, count, 2 * h), BF16),
            pltpu.VMEM((n, shard // 2, 2 * h), BF16),
            pltpu.VMEM((n, shard // 2, 2 * h), BF16),
            pltpu.VMEM((n, 3 * h, width), BF16),
            pltpu.VMEM((n,) + up_weight.shape, BF16),
            pltpu.VMEM((n,) + down_weight.shape, BF16),
            pltpu.VMEM((2, out_width, shard // 2), F32),
            pltpu.VMEM((out_width, shard // 2), F32),
            pltpu.VMEM((n, 2, out_width, shard // 2), BF16),
            dma((n - 1,)), dma((n - 1,)),
            dma((n - 1,)), dma((n - 1,)),
            dma((3, n // 2, 2)), dma((3, n // 2)),
            dma((3, n // 2)), dma((3, n // 2)),
            dma((n,)), dma((n,)),
            dma((3, n)), dma((3, n)),
            dma((2,)),
            dma((n,)), dma((n,)),
            dma((n,)), dma((n,)),
        ],
        compiler_params=pltpu.CompilerParams(
            collective_id=0, has_side_effects=True, vmem_limit_bytes=60 * 1024 * 1024
        ),
    )(tokens, cond, ada_block, ada_final, qkv, out_weight, up_weight, down_weight, final_weight.T)
    return guided.astype(F32).T


def attend(projected):
    token_count = projected.shape[0]
    local_width = projected.shape[2]
    local_heads = local_width // HEAD_SIZE
    per_head = projected.reshape(token_count, 3, local_heads, HEAD_SIZE)
    scores = jnp.einsum(
        "thd,shd->hts", per_head[:, 0], per_head[:, 1], preferred_element_type=jnp.float32
    ) * HEAD_SIZE ** (-0.5)
    softmaxed = jax.nn.softmax(scores, axis=-1)
    values_f = per_head[:, 2].astype(jnp.float32)
    head_out = jnp.einsum("hts,shd->thd", softmaxed, values_f)
    return head_out.reshape(token_count, local_width).astype(jnp.bfloat16)


def split(
    tokens,
    conditions,
    ada_block,
    ada_final,
    qkv_weight,
    out_weight,
    up_weight,
    down_weight,
    final_weight,
):
    model_width = tokens.shape[1]
    signal = jax.nn.silu(conditions).astype(jnp.bfloat16)
    block_local = jnp.dot(signal, ada_block, preferred_element_type=jnp.float32)[0]
    final_local = jnp.dot(signal, ada_final, preferred_element_type=jnp.float32)[0]
    shifts, final_mod = (
        lax.all_gather(block_local, "tp", axis=0, tiled=True),
        lax.all_gather(final_local, "tp", axis=0, tiled=True),
    )
    shifts = shifts.reshape(6, model_width)
    stream = tokens.astype(jnp.float32)
    normed = modulate(stream, shifts[1], shifts[0])
    projected = jnp.einsum(
        "td,dke->tke", normed, qkv_weight, preferred_element_type=jnp.float32
    ).astype(jnp.bfloat16)
    head_out = attend(projected)
    attended = lax.psum(
        jnp.dot(head_out, out_weight, preferred_element_type=jnp.float32).astype(jnp.bfloat16), "tp"
    ).astype(jnp.float32)
    stream = stream + shifts[2] * attended
    normed = modulate(stream, shifts[4], shifts[3])
    upward = jnp.dot(normed, up_weight, preferred_element_type=jnp.float32)
    hidden = jax.nn.gelu(upward, approximate=True).astype(jnp.bfloat16)
    mlp_out = lax.psum(
        jnp.dot(hidden, down_weight, preferred_element_type=jnp.float32).astype(jnp.bfloat16), "tp"
    ).astype(jnp.float32)
    stream = stream + shifts[5] * mlp_out
    final_mod = final_mod.reshape(2, model_width)
    final_in = modulate(stream, final_mod[1], final_mod[0])
    predicted = jnp.dot(final_in, final_weight, preferred_element_type=jnp.float32)
    is_cond = lax.axis_index("cfg") == 0
    weighting = jnp.where(is_cond, guidance, 1.0 - guidance).astype(jnp.float32)
    return lax.psum((weighting * predicted).astype(jnp.bfloat16), "cfg").astype(jnp.float32)


def solution(mesh):
    n = mesh.shape["tp"]

    def local(tokens, cond, ada_block, ada_final, qkv_weight, out_weight, up_weight, down_weight, final_weight):
        args = (tokens, cond, ada_block, ada_final, qkv_weight, out_weight, up_weight, down_weight, final_weight)
        gathered = 2 * n * (out_weight.size + up_weight.size + down_weight.size)
        needed = gathered + 8 * tokens.size + 16 * tokens.shape[0] * HEAD_SIZE
        one_head = qkv_weight.shape[2] == HEAD_SIZE
        fits = needed < 24 * 1024 * 1024 and tokens.shape[0] % (256 * n) == 0
        pairs = mesh.shape["cfg"] == 2 and mesh.shape["dp"] == 2
        if n == 8 and pairs and one_head and fits:
            return fused(n, *args)
        return split(*args)

    placed = (
        P("dp", None),
        P(("dp", "cfg"), None),
        P(None, "tp"),
        P(None, "tp"),
        P(None, None, "tp"),
        P("tp", None),
        P(None, "tp"),
        P("tp", None),
        P(),
    )
    return jax.shard_map(
        local, mesh=mesh, in_specs=placed, out_specs=P("dp", None), check_vma=False
    )
```

```python
import functools
import math

import jax
import jax.numpy as jnp
from jax import lax
from jax.experimental import pallas as pl
from jax.experimental.pallas import tpu as pltpu
from jax.sharding import PartitionSpec as P

HEAD_SIZE = 64
MESH = pl.DeviceIdType.MESH
F32, BF16 = jnp.float32, jnp.bfloat16

SHARE = 10
EARLY = ((0, 1), (1, 1))
QKV_PLAN = {4: ((2, 1), (3, 1)), 7: ((0, 2), (1, 2))}
PLAN = {
    1: ((2, 2), (3, 2)), 2: ((0, 3), (2, 11), (3, 11)), 3: ((1, 3),), 4: ((2, 3), (3, 3)),
    5: ((0, 4), (2, 12), (3, 12)), 6: ((1, 4),), 7: ((2, 4), (2, 13)),
}
LATE = ((3, 4), (3, 13), (2, 14))
LAST = ((3, 14),)

guidance = 4.0
epsilon = 1e-06


def layer_norm(values):
    average = jnp.mean(values, -1, keepdims=True)
    centred = values - average
    spread = jnp.mean(centred * centred, -1, keepdims=True)
    return centred * lax.rsqrt(spread + epsilon)


def modulate(stream, scales, shifts):
    return (layer_norm(stream) * (1.0 + scales) + shifts).astype(BF16)


def dot(a, b):
    return jnp.dot(a, b, preferred_element_type=F32)


def dot_nt(a, b):
    return lax.dot_general(a, b, (((1,), (1,)), ((), ())), preferred_element_type=F32)


def remote(src, dst, send, recv, where):
    return pltpu.make_async_remote_copy(
        src_ref=src, dst_ref=dst, send_sem=send, recv_sem=recv, device_id=where, device_id_type=MESH
    )


def rows_of(ref, start, count):
    return ref.at[pl.ds(pl.multiple_of(start, count), count)]


def block_kernel(
    n,
    tokens, cond, ada_block, ada_final, qkv, out_w, up_w, down_w, final_w,
    result,
    mod_mine, mod_all, xhat, q_s, k_s, v_s, ho_mine, ho_all, f_out, f_up, f_down,
    half_out, half_in, fin_buf,
    mod_send, mod_recv, ho_send, ho_recv, z_send, z_recv, x_send, x_recv, y_send, y_recv, s_send, s_recv, h_sem, p_send, p_recv, d_send, d_recv,
):
    me = lax.axis_index("tp")
    c = lax.axis_index("cfg")
    other = {"cfg": 1 - c}
    count, width = tokens.shape
    shard = count // n
    nz = n // 2
    x, z = lax.rem(me, 2), me // 2

    y = lax.axis_index("dp")
    beside = {"dp": 1 - y}
    across = {"tp": z * 2 + 1 - x}

    barrier = pltpu.get_barrier_semaphore()
    for d in range(1, n):
        pl.semaphore_signal(
            barrier, inc=1, device_id={"tp": lax.rem(me + d, n)}, device_id_type=MESH
        )
    pl.semaphore_signal(barrier, inc=1, device_id=other, device_id_type=MESH)
    pl.semaphore_signal(barrier, inc=1, device_id=beside, device_id_type=MESH)

    raw = cond[...]
    signal = jnp.broadcast_to(raw / (1.0 + jnp.exp(-raw)), (8, raw.shape[1])).astype(BF16)
    nb, nf = ada_block.shape[1], ada_final.shape[1]
    mod_mine[0, :, :nb] = dot(signal, ada_block[...])[0:1]
    mod_mine[0, :, nb:] = dot(signal, ada_final[...])[0:1]
    pl.semaphore_wait(barrier, n + 1)

    def mod_copy(d):
        return remote(
            mod_mine.at[0], mod_all.at[me], mod_send.at[d - 1], mod_recv.at[d - 1],
            {"tp": lax.rem(me + d, n)},
        )

    for d in range(1, n):
        mod_copy(d).start()

    half_up = up_w.shape[0] // 2
    own = (out_w, up_w, up_w, down_w)
    full = (f_out, f_up, f_up, f_down)
    first = (0, 0, half_up, 0)
    extent = (out_w.shape[0], half_up, half_up, down_w.shape[0])
    paired = (False, False, True, True)
    kinds = len(own)
    h = HEAD_SIZE

    def region(ref, k, core, plane=None):
        base, rows = first[k], extent[k]
        if k == 0 and ref is not out_w:
            base = h
        size = rows // 2
        start = base + core * size
        if plane is not None:
            size = size // 2
            start = start + plane * size
        return rows_of(ref, start, size)

    def fetched(k, owner):
        return region(full[k].at[owner], k, c, y if paired[k] else None)

    def z_copy(k, zo, way, mine=False):
        owner = zo * 2 + x
        src = region(own[k], k, c, y if paired[k] else None) if mine else fetched(k, owner)
        return remote(
            src, fetched(k, owner), z_send.at[k, zo, way], z_recv.at[k, zo],
            {"tp": (z + 1 - 2 * way) * 2 + x},
        )

    def x_copy(k, zo, mine=False):
        owner = zo * 2 + x
        src = region(own[k], k, c, y if paired[k] else None) if mine else fetched(k, owner)
        return remote(src, fetched(k, owner), x_send.at[k, zo], x_recv.at[k, zo], across)

    def y_copy(k, owner, plane):
        dst = region(full[k].at[owner], k, c, plane)
        return remote(dst, dst, y_send.at[k, owner], y_recv.at[k, owner], beside)

    def core_copy(k, owner, core):
        dst = region(full[k].at[owner], k, core)
        return remote(dst, dst, s_send.at[k, owner], s_recv.at[k, owner], other)

    def hand_on(k, owner):
        if paired[k]:
            y_copy(k, owner, y).start()
        else:
            core_copy(k, owner, c).start()

    def stage(k, dist):
        if dist > SHARE:
            share(k, dist - SHARE)
            return
        if dist == 0:
            for way in (0, 1):
                @pl.when(z < nz - 1 if way == 0 else z > 0)
                def _():
                    z_copy(k, z, way, True).start()
            x_copy(k, z, True).start()
            return
        for way in (0, 1):
            zo = z - dist if way == 0 else z + dist
            inside = zo >= 0 if way == 0 else zo < nz

            if dist < nz:
                @pl.when(inside)
                def _():
                    z_copy(k, zo, way).wait_recv()
                    @pl.when(z < nz - 1 if way == 0 else z > 0)
                    def _():
                        z_copy(k, zo, way).start()
                    x_copy(k, zo).start()
                    hand_on(k, zo * 2 + x)

            zx = z - dist + 1 if way == 0 else z + dist - 1
            if dist > 1 or way == 0:
                @pl.when(zx >= 0 if way == 0 else zx < nz)
                def _():
                    place = fetched(k, zx * 2 + 1 - x)
                    remote(place, place, x_send.at[k, zx], x_recv.at[k, zx], across).wait_recv()
                    hand_on(k, zx * 2 + 1 - x)

    def steps_at(plan, i):
        for when, steps in plan.items():
            @pl.when(i == when)
            def _():
                for k, dist in steps:
                    stage(k, dist)

    def share(k, dist):
        def one(owner):
            y_copy(k, owner, 1 - y).wait_recv()
            core_copy(k, owner, c).start()

        for way in (0, 1):
            zo = z - dist if way == 0 else z + dist
            if dist < nz:
                @pl.when(zo >= 0 if way == 0 else zo < nz)
                def _():
                    one(zo * 2 + x)
            zx = z - dist + 1 if way == 0 else z + dist - 1
            if dist > 1 or way == 0:
                @pl.when(zx >= 0 if way == 0 else zx < nz)
                def _():
                    one(zx * 2 + 1 - x)

    def arrived(k):
        for d in range(1, n):
            core_copy(k, lax.rem(me + d, n), 1 - c).wait_recv()

    for k in range(kinds):
        stage(k, 0)
    empty = jnp.zeros((h, width), BF16)
    for t in range(n):
        f_out[t, :h] = empty
        f_out[t, 2 * h :] = empty
    f_out[me, h : 2 * h] = out_w[...]
    f_up[me] = up_w[...]
    f_down[me] = down_w[...]

    def norm_step(i, _):
        r = pl.ds(pl.multiple_of(i * shard, shard), shard)
        xhat[r, :] = layer_norm(tokens[r, :].astype(F32))
        return 0

    lax.fori_loop(0, count // shard, norm_step, 0)

    mod_all[me] = mod_mine[0]
    for d in range(1, n):
        origin = mod_all.at[lax.rem(me - d + n, n)]
        remote(origin, origin, mod_send.at[d - 1], mod_recv.at[d - 1], across).wait_recv()

    def mod_row(base, per, row):
        lane = math.gcd(per, width)
        pieces = []
        for g in range(row * width // lane, (row + 1) * width // lane):
            t, off = (g * lane) // per, (g * lane) % per
            pieces.append(mod_all[t, :, base + off : base + off + lane])
        return jnp.concatenate(pieces, axis=1)

    shift1, scale1, gate1, shift2, scale2, gate2 = [mod_row(0, nb, r) for r in range(6)]
    shift_f, scale_f = [mod_row(nb, nf, r) for r in range(2)]

    lanes = lax.broadcasted_iota(jnp.int32, (shard, 2 * h), 1)
    upper = (lanes >= h).astype(F32)
    v_w, none = qkv[2], jnp.zeros((h, width), BF16)
    v_low = jnp.concatenate([v_w, none], axis=0)
    v_high = jnp.concatenate([none, v_w], axis=0)

    for k, dist in EARLY:
        stage(k, dist)

    def qkv_step(i, _):
        steps_at(QKV_PLAN, i)
        r = pl.ds(pl.multiple_of(i * shard, shard), shard)
        normed = (xhat[r, :] * (1.0 + scale1) + shift1).astype(BF16)
        q_s[r, :] = (dot_nt(normed, qkv[0]) * (h ** -0.5 * math.log2(math.e))).astype(BF16)
        k_s[r, :] = dot_nt(normed, qkv[1]).astype(BF16)
        v_s[0, r, :] = (dot_nt(normed, v_low) + upper).astype(BF16)
        v_s[1, r, :] = (dot_nt(normed, v_high) + (1.0 - upper)).astype(BF16)
        return 0

    lax.fori_loop(0, count // shard, qkv_step, 0)

    def ho_copy(i):
        return remote(
            ho_mine.at[i], ho_all.at[me], ho_send.at[i], ho_recv.at[i],
            {"tp": lax.rem(me + 1 + i, n)},
        )

    sub = shard // 2

    def attend_step(i, _):
        steps_at(PLAN, i)

        peer = lax.rem(me + 1 + i, n)
        parts = []
        for part in range(2):
            r = pl.ds(pl.multiple_of(peer * shard + part * sub, sub), sub)
            scores = dot_nt(q_s[r, :], k_s[...])
            top = jnp.max(scores, axis=-1, keepdims=True)
            weights = jnp.exp2(scores - top).astype(BF16)
            mixed = dot(weights, v_s[part])
            total = mixed[:, h : h + 1] if part == 0 else mixed[:, 0:1]
            parts.append(mixed / total)
        ho_mine[i] = jnp.where(lanes[:sub] < h, parts[0], parts[1]).astype(BF16)

        @pl.when(i < n - 1)
        def _():
            ho_copy(i).start()

        return 0

    lax.fori_loop(0, n, attend_step, 0)
    for k, dist in LATE:
        stage(k, dist)

    ho_all[me] = ho_mine[n - 1]
    arrived(0)
    for i in range(n - 1):
        origin = ho_all.at[lax.rem(me - 1 - i + n, n)]
        remote(origin, origin, ho_send.at[i], ho_recv.at[i], across).wait_recv()
    def project(lo):
        sums = dot(ho_all[0], f_out[0, lo : lo + 2 * h])
        for t in range(1, n):
            sums += dot(ho_all[t], f_out[t, lo : lo + 2 * h])
        return sums

    attended = jnp.concatenate([project(h), project(0)], axis=0)
    r = pl.ds(pl.multiple_of(me * shard, shard), shard)
    stream = tokens[r, :].astype(F32) + gate1 * attended
    normed = modulate(stream, scale2, shift2)
    arrived(1)
    arrived(2)
    hidden = [
        jax.nn.gelu(dot(normed, f_up[t]), approximate=True).astype(BF16) for t in range(n)
    ]
    for k, dist in LAST:
        stage(k, dist)
    arrived(3)
    mlp = dot(hidden[0], f_down[0])
    for t in range(1, n):
        mlp += dot(hidden[t], f_down[t])
    stream = stream + gate2 * mlp
    final_in = modulate(stream, scale_f, shift_f)

    weighting = jnp.where(c == 0, guidance, 1.0 - guidance).astype(F32)
    predicted = weighting * dot_nt(final_w[...], final_in)
    part = shard // 2
    for half in range(2):
        half_out[half] = predicted[:, half * part : (half + 1) * part]
    trade = remote(half_out.at[1 - c], half_in, h_sem.at[0], h_sem.at[1], other)
    trade.start()
    trade.wait()
    fin_buf[me, c] = (half_out[c] + half_in[...]).astype(BF16)

    def push(d):
        return remote(
            fin_buf.at[me, c], fin_buf.at[me, c], p_send.at[d], p_recv.at[d],
            {"tp": lax.rem(me + d, n)},
        )

    def hand(d, core):
        place = fin_buf.at[lax.rem(me - d + n, n), core]
        return remote(place, place, d_send.at[d], d_recv.at[d], other)

    for d in (4, 3, 5, 2, 6, 1, 7):
        if d < n:
            push(d).start()
    hand(0, c).start()
    for d in range(1, n):
        place = fin_buf.at[lax.rem(me - d + n, n), c]
        remote(place, place, p_send.at[d], p_recv.at[d], across).wait_recv()
        hand(d, c).start()
    for d in range(n):
        hand(d, 1 - c).wait_recv()
    for t in range(n):
        for half in range(2):
            lo = t * shard + half * part
            result[:, lo : lo + part] = fin_buf[t, half]

    for d in range(1, n):
        mod_copy(d).wait_send()
        push(d).wait_send()
        ho_copy(d - 1).wait_send()
    for d in range(n):
        hand(d, c).wait_send()
    for k in range(kinds):
        for zo in range(nz):
            x_copy(k, zo).wait_send()
        for way in (0, 1):
            @pl.when(z < nz - 1 if way == 0 else z > 0)
            def _():
                for dist in range(nz):
                    zo = z - dist if way == 0 else z + dist
                    @pl.when(zo >= 0 if way == 0 else zo < nz)
                    def _():
                        z_copy(k, zo, way).wait_send()
        for d in range(1, n):
            core_copy(k, lax.rem(me + d, n), c).wait_send()
        for d in range(1, n):
            if paired[k]:
                y_copy(k, lax.rem(me + d, n), y).wait_send()


def fused(n, tokens, cond, ada_block, ada_final, qkv_weight, out_weight, up_weight, down_weight, final_weight):
    count, width = tokens.shape
    shard = count // n
    qkv = jnp.transpose(qkv_weight, (1, 2, 0))
    mod = ada_block.shape[1] + ada_final.shape[1]
    h, out_width = HEAD_SIZE, final_weight.shape[1]
    dma = pltpu.SemaphoreType.DMA
    vm = pl.BlockSpec(memory_space=pltpu.VMEM)
    guided = pl.pallas_call(
        functools.partial(block_kernel, n),
        out_shape=jax.ShapeDtypeStruct((out_width, count), BF16),
        in_specs=[vm] * 9,
        out_specs=vm,
        scratch_shapes=[
            pltpu.VMEM((1, 1, mod), F32),
            pltpu.VMEM((n, 1, mod), F32),
            pltpu.VMEM((count, width), F32),
            pltpu.VMEM((count, h), BF16),
            pltpu.VMEM((count, h), BF16),
            pltpu.VMEM((2, count, 2 * h), BF16),
            pltpu.VMEM((n, shard // 2, 2 * h), BF16),
            pltpu.VMEM((n, shard // 2, 2 * h), BF16),
            pltpu.VMEM((n, 3 * h, width), BF16),
            pltpu.VMEM((n,) + up_weight.shape, BF16),
            pltpu.VMEM((n,) + down_weight.shape, BF16),
            pltpu.VMEM((2, out_width, shard // 2), F32),
            pltpu.VMEM((out_width, shard // 2), F32),
            pltpu.VMEM((n, 2, out_width, shard // 2), BF16),
            dma((n - 1,)), dma((n - 1,)),
            dma((n - 1,)), dma((n - 1,)),
            dma((4, n // 2, 2)), dma((4, n // 2)),
            dma((4, n // 2)), dma((4, n // 2)),
            dma((4, n)), dma((4, n)),
            dma((4, n)), dma((4, n)),
            dma((2,)),
            dma((n,)), dma((n,)),
            dma((n,)), dma((n,)),
        ],
        compiler_params=pltpu.CompilerParams(
            collective_id=0, has_side_effects=True, vmem_limit_bytes=60 * 1024 * 1024
        ),
    )(tokens, cond, ada_block, ada_final, qkv, out_weight, up_weight, down_weight, final_weight.T)
    return guided.astype(F32).T


def attend(projected):
    token_count = projected.shape[0]
    local_width = projected.shape[2]
    local_heads = local_width // HEAD_SIZE
    per_head = projected.reshape(token_count, 3, local_heads, HEAD_SIZE)
    scores = jnp.einsum(
        "thd,shd->hts", per_head[:, 0], per_head[:, 1], preferred_element_type=jnp.float32
    ) * HEAD_SIZE ** (-0.5)
    softmaxed = jax.nn.softmax(scores, axis=-1)
    values_f = per_head[:, 2].astype(jnp.float32)
    head_out = jnp.einsum("hts,shd->thd", softmaxed, values_f)
    return head_out.reshape(token_count, local_width).astype(jnp.bfloat16)


def split(
    tokens,
    conditions,
    ada_block,
    ada_final,
    qkv_weight,
    out_weight,
    up_weight,
    down_weight,
    final_weight,
):
    model_width = tokens.shape[1]
    signal = jax.nn.silu(conditions).astype(jnp.bfloat16)
    block_local = jnp.dot(signal, ada_block, preferred_element_type=jnp.float32)[0]
    final_local = jnp.dot(signal, ada_final, preferred_element_type=jnp.float32)[0]
    shifts, final_mod = (
        lax.all_gather(block_local, "tp", axis=0, tiled=True),
        lax.all_gather(final_local, "tp", axis=0, tiled=True),
    )
    shifts = shifts.reshape(6, model_width)
    stream = tokens.astype(jnp.float32)
    normed = modulate(stream, shifts[1], shifts[0])
    projected = jnp.einsum(
        "td,dke->tke", normed, qkv_weight, preferred_element_type=jnp.float32
    ).astype(jnp.bfloat16)
    head_out = attend(projected)
    attended = lax.psum(
        jnp.dot(head_out, out_weight, preferred_element_type=jnp.float32).astype(jnp.bfloat16), "tp"
    ).astype(jnp.float32)
    stream = stream + shifts[2] * attended
    normed = modulate(stream, shifts[4], shifts[3])
    upward = jnp.dot(normed, up_weight, preferred_element_type=jnp.float32)
    hidden = jax.nn.gelu(upward, approximate=True).astype(jnp.bfloat16)
    mlp_out = lax.psum(
        jnp.dot(hidden, down_weight, preferred_element_type=jnp.float32).astype(jnp.bfloat16), "tp"
    ).astype(jnp.float32)
    stream = stream + shifts[5] * mlp_out
    final_mod = final_mod.reshape(2, model_width)
    final_in = modulate(stream, final_mod[1], final_mod[0])
    predicted = jnp.dot(final_in, final_weight, preferred_element_type=jnp.float32)
    is_cond = lax.axis_index("cfg") == 0
    weighting = jnp.where(is_cond, guidance, 1.0 - guidance).astype(jnp.float32)
    return lax.psum((weighting * predicted).astype(jnp.bfloat16), "cfg").astype(jnp.float32)


def solution(mesh):
    n = mesh.shape["tp"]

    def local(tokens, cond, ada_block, ada_final, qkv_weight, out_weight, up_weight, down_weight, final_weight):
        args = (tokens, cond, ada_block, ada_final, qkv_weight, out_weight, up_weight, down_weight, final_weight)
        gathered = 2 * n * (out_weight.size + up_weight.size + down_weight.size)
        needed = gathered + 8 * tokens.size + 16 * tokens.shape[0] * HEAD_SIZE
        one_head = qkv_weight.shape[2] == HEAD_SIZE
        fits = needed < 24 * 1024 * 1024 and tokens.shape[0] % (256 * n) == 0
        pairs = mesh.shape["cfg"] == 2 and mesh.shape["dp"] == 2
        if n == 8 and pairs and one_head and fits:
            return fused(n, *args)
        return split(*args)

    placed = (
        P("dp", None),
        P(("dp", "cfg"), None),
        P(None, "tp"),
        P(None, "tp"),
        P(None, None, "tp"),
        P("tp", None),
        P(None, "tp"),
        P("tp", None),
        P(),
    )
    return jax.shard_map(
        local, mesh=mesh, in_specs=placed, out_specs=P("dp", None), check_vma=False
    )
```
